256 devices in a mesh: tok: 8 (over x, core), voc: 32 (over z, y).
Axes of the slice: x: 4, y: 4, z: 8, core: 2. Of those that a mesh axis runs over, the one named last changes fastest.
Arguments:
- hidden_rows: bfloat16 [1024, 8192], P('tok', 'voc'), may hold values from -2 to 2
- teacher_weight: bfloat16 [8192, 152064], P(None, ('tok', 'voc')), may hold values from -64 to 64
- student_logits: bfloat16 [1024, 128256], P('tok', 'voc'), may hold values from -8 to 300
- slot_source: int32 [32, 32, 256], P('voc'), may hold values from -1 to 4751, as said below
- slot_target: int32 [32, 32, 256], P('voc'), may hold values from -1 to 4007, as said below
Outputs:
- loss: float32 [1024], P('tok')
- student_grad: bfloat16 [1024, 128256], P('tok', 'voc')
The draws below stay inside these ranges and needn't reach their ends.
Inputs may be any that keep to these rules, and one draw needn't show every extreme that they name: Each of the 4752 local columns of group g appears in exactly one slot of slot_source[g]; all other slots hold -1. One owner's 256 slots are filled in every group. slot_target[j, g, c] is -1 exactly where slot_source[g, j, c] is -1.
All inputs are finite; a program needn't handle non-finite values.
Results may differ from the reference program's by a relative error of at most 0.0022.
The reference program's roundings to bfloat16 on the way (of `probs`) count: a program that leaves them out, or rounds other values in their place, can miss the bound.
Values may be sent and summed in bfloat16 or wider, within the bound.
No kernel may reach another device: no remote copies, remote signals or barrier semaphores. Data moves between devices by JAX's collectives and lax.ppermute only.
A program may use at most 128 MiB of HBM per device.

```python
import math
import jax
import jax.numpy as jnp

D = 8192
V = 152064
S = 128256
TOKENS = 1024
GROUP = 4752
SL = 4008
CAP = 256
N_TOK = 8
N_VOC = 32


def hidden_parts(key):
    noise = jnp.clip(jax.random.normal(jax.random.fold_in(key, 11), (TOKENS, D), jnp.float32), -6.0, 6.0)
    common = jnp.clip(jax.random.normal(jax.random.fold_in(key, 13), (D,), jnp.float32), -6.0, 6.0)
    scale = jnp.ones((TOKENS, 1), jnp.float32)
    rows = 0.1 * scale * noise + 0.1 * common[None, :]
    rows = rows.astype(jnp.bfloat16).astype(jnp.float32)
    return (rows, common)


def draw_hidden_rows(key, part):
    return hidden_parts(key)[0].astype(jnp.bfloat16)


def aimed_columns(rows, common, strength):
    along = jnp.sum(rows * common[None, :], axis=1) / jnp.sum(common * common)
    apart = rows - along[:, None] * common[None, :]
    reach = jnp.sum(apart * rows, axis=1)
    return (apart * (strength / reach)[:, None]).T


def draw_teacher_weight(key, part):
    rows, common = hidden_parts(key)
    base = jnp.clip(jax.random.normal(jax.random.fold_in(key, 21), (D, V), jnp.float32), -6.0, 6.0)
    slope = 0.8 + 0.4 * jnp.arange(V, dtype=jnp.float32) / V
    weight = base * slope[None, :] * (3.0 / math.sqrt(D))
    offset = math.log(3.0) * jnp.arange(V, dtype=jnp.float32) / V
    lift = common / (0.1 * jnp.sum(common * common))
    weight = weight + lift[:, None] * offset[None, :]
    columns = jax.random.permutation(jax.random.fold_in(key, 23), V)
    leading = jax.random.uniform(jax.random.fold_in(key, 24), (TOKENS,), jnp.float32, 8.5, 10.0)
    weight = weight.at[:, columns[:TOKENS]].set(aimed_columns(rows, common, leading))
    weight = jnp.clip(weight, -64.0, 64.0)
    return weight.astype(jnp.bfloat16)


def draw_student_logits(key, part):
    base = jnp.clip(jax.random.normal(jax.random.fold_in(key, 31), (TOKENS, S), jnp.float32), -4.0, 4.0)
    slope = 1.0 + 0.5 * jnp.arange(S, dtype=jnp.float32) / S
    values = base * slope[None, :]
    return values.astype(jnp.bfloat16)


def fold_plan(key):
    slot_positions = N_VOC * CAP
    fullest = jax.random.randint(jax.random.fold_in(key, 41), (), 0, N_VOC)
    holder_device = jnp.arange(slot_positions, dtype=jnp.int32) // CAP
    position_index = jnp.arange(slot_positions, dtype=jnp.int32)

    def one_group(group):
        cluster_key = jax.random.fold_in(jax.random.fold_in(key, 42), group)
        extra_reward = jax.random.randint(jax.random.fold_in(cluster_key, 1), (N_VOC,), 0, 4096)
        random_jitter = jax.random.randint(jax.random.fold_in(cluster_key, 2), (slot_positions,), 0, 4096)
        ranking_score = (random_jitter + extra_reward[holder_device]) * slot_positions + position_index
        ranking_score = jnp.where(holder_device == fullest, 8192 * slot_positions + position_index, ranking_score)
        order = jnp.argsort(-ranking_score, stable=True)
        chosen = order[:GROUP]
        columns = jax.random.permutation(jax.random.fold_in(cluster_key, 3), GROUP).astype(jnp.int32)
        source = jnp.full((slot_positions,), -1, jnp.int32).at[chosen].set(columns)
        target = jax.random.randint(jax.random.fold_in(cluster_key, 4), (slot_positions,), 0, SL)
        target = jnp.where(source >= 0, target, -1).astype(jnp.int32)
        return (source.reshape(N_VOC, CAP), target.reshape(N_VOC, CAP))
    return jax.vmap(one_group)(jnp.arange(N_VOC, dtype=jnp.int32))


def draw_slot_source(key, part):
    return fold_plan(key)[0]


def draw_slot_target(key, part):
    return jnp.transpose(fold_plan(key)[1], (1, 0, 2))


def setup_inputs(seed: int = 0) -> dict:
    key_list = jax.random.split(jax.random.key(seed), 6)
    hidden_rows = draw_hidden_rows(jax.random.fold_in(key_list[5], 71), 0)
    teacher_weight = draw_teacher_weight(jax.random.fold_in(key_list[5], 71), 0)
    student_logits = draw_student_logits(jax.random.fold_in(key_list[5], 71), 0)
    slot_source = draw_slot_source(jax.random.fold_in(key_list[5], 71), 0)
    slot_target = draw_slot_target(jax.random.fold_in(key_list[5], 71), 0)
    return {"hidden_rows": hidden_rows, "teacher_weight": teacher_weight, "student_logits": student_logits, "slot_source": slot_source, "slot_target": slot_target}


def reference(hidden_rows, teacher_weight, student_logits, slot_source, slot_target):
    logits = jnp.dot(hidden_rows, teacher_weight, preferred_element_type=jnp.float32)
    teacher_max = jnp.max(logits, axis=1)
    shifted = jnp.exp(logits - teacher_max[:, None])
    teacher_total = jnp.sum(shifted, axis=1)
    probs = (shifted / teacher_total[:, None]).astype(jnp.bfloat16)
    shard_cols = V // (N_TOK * N_VOC)
    owner_cols = S // N_VOC
    groups = jnp.arange(N_VOC, dtype=jnp.int32)[:, None, None]
    owners = jnp.arange(N_VOC, dtype=jnp.int32)[None, :, None]
    valid = slot_source >= 0
    local = jnp.maximum(slot_source, 0)
    entry = ((local // shard_cols) * N_VOC + groups) * shard_cols + local % shard_cols
    target = jnp.transpose(slot_target, (1, 0, 2))
    column = jnp.where(valid, owners * owner_cols + target, S).astype(jnp.int32)
    picked = jnp.take(probs, entry.reshape(-1).astype(jnp.int32), axis=1)
    picked = jnp.where(valid.reshape(-1)[None, :], picked, jnp.zeros_like(picked))
    folded = jnp.zeros((probs.shape[0], S), jnp.float32).at[:, column.reshape(-1)].add(picked.astype(jnp.float32), mode="drop")
    student = student_logits.astype(jnp.float32)
    student_max = jnp.max(student, axis=1)
    student_lse = student_max + jnp.log(jnp.sum(jnp.exp(student - student_max[:, None]), axis=1))
    loss = -jnp.sum(folded * (student - student_lse[:, None]), axis=1)
    student_grad = (jnp.exp(student - student_lse[:, None]) - folded).astype(jnp.bfloat16)
    return loss, student_grad
```

```python
import jax
import jax.numpy as jnp
from jax import lax
from jax.experimental import pallas as pl
from jax.experimental.pallas import tpu as pltpu
from jax.sharding import Mesh
from jax.sharding import PartitionSpec as P

VOC = ("voc_0", "voc_1")
TOK = ("tok_0", "tok_1")
TOK_VOC = ("tok_0", "tok_1", "voc_0", "voc_1")
LOW = -1e30
CHUNKS = 2
ACCS = 8


def from_neighbour(value, axis, step):
    n = lax.axis_size(axis)
    return lax.ppermute(value, axis, [((i + step) % n, i) for i in range(n)])


def ring(value, axis):
    n = lax.axis_size(axis)
    found, up, down = {0: value}, value, value
    for k in range(1, n // 2):
        up, down = from_neighbour(up, axis, 1), from_neighbour(down, axis, -1)
        found[k], found[n - k] = up, down
    half = value.shape[0] // 2
    found[n // 2] = jnp.concatenate(
        [from_neighbour(up[:half], axis, 1), from_neighbour(down[half:], axis, -1)], axis=0
    )
    return jnp.stack([found[k] for k in range(n)])


def logits_kernel(nz, ny, cols, padded, place, *refs):
    first, second = refs[:ny], refs[ny : 2 * ny]
    own_w, other_w, stay, up, down, own_sum, other_sum = refs[2 * ny :]
    step = pl.program_id(0)

    @pl.when(step == 0)
    def _():
        own_sum[...] = jnp.zeros_like(own_sum)
        other_sum[...] = jnp.zeros_like(other_sum)

    parts = []
    for a, b in zip(first, second):
        rows = jnp.concatenate([a[0, 0], b[0, 0]], axis=1)
        parts.append(rows.reshape(-1, rows.shape[-1]))
    rows = jnp.concatenate(parts, axis=1)
    contract = (((1,), (1,)), ((), ()))
    own_sum[...] += lax.dot_general(own_w[...], rows, contract, preferred_element_type=jnp.float32)
    other_sum[...] += lax.dot_general(other_w[...], rows, contract, preferred_element_type=jnp.float32)

    @pl.when(step == nz - 1)
    def _():
        lanes = stay.shape[1]

        def put(out, at, total, block):
            out[at + (padded - 8) : at + padded, :] = jnp.full((8, lanes), LOW, jnp.float32)
            out[at : at + cols, :] = total[:, block * lanes : (block + 1) * lanes]

        put(stay, 0, own_sum, 0)
        put(stay, padded, other_sum, 0)
        put(up, 0, own_sum, 3)
        put(up, padded, other_sum, 3)
        put(up, 2 * padded, own_sum, 2)
        put(down, 0, own_sum, 1)
        put(down, padded, other_sum, 1)
        put(down, 2 * padded, other_sum, 2)


def logits_of(first, second, own_w, other_w, place, padded):
    nz, ny, nx, half, width = first.shape
    cols = own_w.shape[0]
    lanes = 2 * half

    def first_piece(j):
        return pl.BlockSpec(
            (1, 1, nx, half, width), lambda k, s: (k, lax.rem(j + ny - s[1], ny), 0, 0, 0)
        )

    def second_piece(j):
        return pl.BlockSpec(
            (1, 1, nx, half, width), lambda k, s: (lax.rem(j + ny - s[1], ny), k, 0, 0, 0)
        )

    weight = pl.BlockSpec((cols, ny * width), lambda k, s: (0, lax.rem(s[0] + k, nz)))

    def whole(rows):
        return pl.BlockSpec((rows, lanes), lambda k, s: (0, 0))

    def shape(rows):
        return jax.ShapeDtypeStruct((rows, lanes), jnp.float32)

    def body(place, *refs):
        logits_kernel(nz, ny, cols, padded, place, *refs)

    return pl.pallas_call(
        body,
        grid_spec=pltpu.PrefetchScalarGridSpec(
            num_scalar_prefetch=1,
            grid=(nz,),
            in_specs=[first_piece(j) for j in range(ny)]
            + [second_piece(j) for j in range(ny)]
            + [weight, weight],
            out_specs=[whole(2 * padded), whole(3 * padded), whole(3 * padded)],
            scratch_shapes=[pltpu.VMEM((cols, nx * lanes), jnp.float32)] * 2,
        ),
        out_shape=[shape(2 * padded), shape(3 * padded), shape(3 * padded)],
        compiler_params=pltpu.CompilerParams(dimension_semantics=("arbitrary",)),
        name="logits",
    )(place, *([first] * ny), *([second] * ny), own_w, other_w)


def gather_kernel(index, table, out):
    def some(i, carry):
        base = i * 16
        for k in range(16):
            out[pl.ds(base + k, 1), :] = table[pl.ds(index[base + k], 1), :]
        return carry

    lax.fori_loop(0, out.shape[0] // 16, some, 0)


def rows_of(table, index):
    return pl.pallas_call(
        gather_kernel,
        in_specs=[
            pl.BlockSpec(memory_space=pltpu.SMEM),
            pl.BlockSpec(memory_space=pltpu.VMEM),
        ],
        out_specs=pl.BlockSpec(memory_space=pltpu.VMEM),
        out_shape=jax.ShapeDtypeStruct((index.shape[0], table.shape[1]), table.dtype),
        name="rows",
    )(index, table)


def scatter_kernel(target, values, out, wide, *sums):
    wide[...] = values[...].astype(jnp.float32)
    for total in sums:
        total[...] = jnp.zeros_like(total)

    def some(i, carry):
        base = i * (2 * ACCS)
        for turn in range(2):
            at = [target[base + turn * ACCS + k] for k in range(ACCS)]
            new = [
                total[pl.ds(at[k], 1), :] + wide[pl.ds(base + turn * ACCS + k, 1), :]
                for k, total in enumerate(sums)
            ]
            for k, total in enumerate(sums):
                total[pl.ds(at[k], 1), :] = new[k]
        return carry

    lax.fori_loop(0, values.shape[0] // (2 * ACCS), some, 0)
    rows = out.shape[0]
    parts = [total[:rows, :] for total in sums]
    while len(parts) > 1:
        parts = [a + b for a, b in zip(parts[::2], parts[1::2])]
    out[...] = parts[0]


def added_rows(values, target, rows):
    lanes = values.shape[1]
    return pl.pallas_call(
        scatter_kernel,
        in_specs=[
            pl.BlockSpec(memory_space=pltpu.SMEM),
            pl.BlockSpec(memory_space=pltpu.VMEM),
        ],
        out_specs=pl.BlockSpec(memory_space=pltpu.VMEM),
        out_shape=jax.ShapeDtypeStruct((rows, lanes), jnp.float32),
        scratch_shapes=[pltpu.VMEM(values.shape, jnp.float32)]
        + [pltpu.VMEM((rows + 8, lanes), jnp.float32)] * ACCS,
        name="folded",
    )(target, values)


def from_all(value, axes):
    copies = jnp.broadcast_to(value, (lax.axis_size(axes), *value.shape))
    return lax.all_to_all(copies, axes, split_axis=0, concat_axis=0, tiled=True)


def shards(hidden_rows, teacher_weight, student_logits, slot_source, slot_target):
    x, core = lax.axis_index("tok_0"), lax.axis_index("tok_1")
    z, y = lax.axis_index("voc_0"), lax.axis_index("voc_1")
    cols = teacher_weight.shape[1]
    padded = -(-cols // 8) * 8
    own_w = teacher_weight.T
    other_w = lax.ppermute(own_w, "tok_1", [(0, 1), (1, 0)])

    half = hidden_rows.shape[0] // 2
    blocks = ring(hidden_rows, "tok_0")
    first = ring(ring(blocks[:, :half], "voc_1"), "voc_0")
    second = ring(ring(blocks[:, half:], "voc_0"), "voc_1")
    stay, up, down = logits_of(
        first, second, own_w, other_w, jnp.stack([z, y]).astype(jnp.int32), padded
    )

    up = from_neighbour(up, "tok_0", 1)
    down = from_neighbour(down, "tok_0", -1)
    far_up = from_neighbour(up[2 * padded :], "tok_0", 1)
    far_down = from_neighbour(down[2 * padded :], "tok_0", -1)
    lanes = stay.shape[1]
    table = jnp.concatenate(
        [
            stay,
            up[: 2 * padded],
            far_up,
            far_down,
            down[: 2 * padded],
            jnp.full((8, lanes), LOW, jnp.float32),
        ],
        axis=0,
    )

    source = slot_source[0]
    owners, slots = source.shape
    shard = jnp.maximum(source, 0) // cols
    local = jnp.maximum(source, 0) - shard * cols
    block = (shard // 2 - x + 4) % 4
    side = (shard % 2) ^ core
    index = jnp.where(source >= 0, block * (2 * padded) + side * padded + local, 8 * padded)
    width = student_logits.shape[1]
    target = jnp.where(slot_target[0] >= 0, slot_target[0], width)
    some = slots // CHUNKS
    picked = [
        rows_of(table, index[:, i * some : (i + 1) * some].reshape(-1).astype(jnp.int32))
        for i in range(CHUNKS)
    ]

    student = student_logits.T.astype(jnp.float32)
    student_max = jnp.max(student, axis=0)
    student_total = jnp.sum(jnp.exp(student - student_max[None]), axis=0)
    own_max = jnp.max(table, axis=0)
    own_total = jnp.sum(jnp.exp(table - own_max[None]), axis=0)
    stats = from_all(jnp.stack([own_max, own_total, student_max, student_total]), VOC)
    teacher_max = jnp.max(stats[:, 0], axis=0)
    teacher_total = jnp.sum(stats[:, 1] * jnp.exp(stats[:, 0] - teacher_max[None]), axis=0)
    highest = jnp.max(stats[:, 2], axis=0)
    student_lse = highest + jnp.log(
        jnp.sum(stats[:, 3] * jnp.exp(stats[:, 2] - highest[None]), axis=0)
    )

    folded = jnp.zeros((width, lanes), jnp.float32)
    for i in range(CHUNKS):
        probs = (jnp.exp(picked[i] - teacher_max[None]) / teacher_total[None]).astype(jnp.bfloat16)
        arrived = lax.all_to_all(
            probs.reshape(owners, some, lanes), VOC, split_axis=0, concat_axis=0, tiled=True
        )
        goal = target[:, i * some : (i + 1) * some].reshape(-1).astype(jnp.int32)
        folded = folded + added_rows(arrived.reshape(-1, lanes), goal, width)

    sums = from_all(jnp.stack([jnp.sum(folded * student, axis=0), jnp.sum(folded, axis=0)]), VOC)
    cross, mass = jnp.sum(sums[:, 0], axis=0), jnp.sum(sums[:, 1], axis=0)
    loss = student_lse * mass - cross
    student_grad = (jnp.exp(student - student_lse[None]) - folded).astype(jnp.bfloat16)
    return (loss, student_grad.T)


def solution(mesh):
    finer = Mesh(mesh.devices.reshape(4, 2, 8, 4), ("tok_0", "tok_1", "voc_0", "voc_1"))
    placed = (P(TOK, VOC), P(None, TOK_VOC), P(TOK, VOC), P(VOC, None, None), P(VOC, None, None))
    return jax.shard_map(
        shards, mesh=finer, in_specs=placed, out_specs=(P(TOK), P(TOK, VOC)), check_vma=False
    )
```

```python
import jax
import jax.numpy as jnp
from jax import lax
from jax.experimental import pallas as pl
from jax.experimental.pallas import tpu as pltpu
from jax.sharding import Mesh
from jax.sharding import PartitionSpec as P


VOC = ("voc_0", "voc_1")
TOK = ("tok_0", "tok_1")
TOK_VOC = ("tok_0", "tok_1", "voc_0", "voc_1")
LOW = -1e30
CHUNKS = 2
ACCS = 8
STEP = 120


def from_neighbour(value, axis, step):
    n = lax.axis_size(axis)
    return lax.ppermute(value, axis, [((i + step) % n, i) for i in range(n)])


def ring(value, axis):
    n = lax.axis_size(axis)
    found, up, down = {0: [value]}, value, value
    for k in range(1, n // 2):
        up, down = from_neighbour(up, axis, 1), from_neighbour(down, axis, -1)
        found[k], found[n - k] = [up], [down]
    half = value.shape[0] // 2
    found[n // 2] = [
        from_neighbour(up[:half], axis, 1), from_neighbour(down[half:], axis, -1)
    ]
    return [found[k] for k in range(n)]


def stacked(found):
    return jnp.stack([f[0] if len(f) == 1 else jnp.concatenate(f, axis=0) for f in found])


def half_swapped(first, second, low):
    half = first.shape[1] // 2
    return (
        jnp.where(low, first, pltpu.roll(second, half, 1)),
        jnp.where(low, pltpu.roll(first, half, 1), second),
    )


def logits_kernel(nz, counts, cols, near, row, place, *refs):
    ny, at = len(counts), sum(counts)
    pieces = iter(refs[:at])
    own_w, other_w, before, *outs, stats, own_sum, other_sum, ordered = refs[at:]
    step = pl.program_id(0)

    @pl.when(step == 0)
    def _():
        own_sum[...] = jnp.zeros_like(own_sum)
        other_sum[...] = jnp.zeros_like(other_sum)

    rows, width = [], ordered.shape[-1]
    for j, count in enumerate(counts):
        parts = [next(pieces)[...].reshape(-1, width) for _ in range(count)]
        rows.append(parts[0] if count == 1 else jnp.concatenate(parts, axis=0))
        if near != 0:
            ordered[lax.rem(place[1] + j, ny), :, :] = rows[j]
    if near != 0:
        rows = [ordered[j, :, :] for j in range(ny)]
    rows = jnp.concatenate(rows, axis=1)
    contract = (((1,), (1,)), ((), ()))
    for weight, total in ((own_w, own_sum), (other_w, other_sum)):
        total[:cols, :] += lax.dot_general(
            weight[...], rows, contract, preferred_element_type=jnp.float32
        )

    @pl.when(step == nz - 1)
    def _():
        padded = own_sum.shape[0]
        lanes = own_sum.shape[1] // 2
        low = lax.broadcasted_iota(jnp.int32, (STEP, lanes), 1) < lanes // 2
        goals = [lax.rem(place[2] + block, 4) for block in range(4)]

        def spots(at, far, base):
            if near == 0:
                return [outs[0].at[goal, pl.ds(at, STEP), :] for goal in goals]
            stay, up, down = outs
            return [
                stay.at[pl.ds(at, STEP), :],
                down.at[pl.ds(at, STEP), :],
                far.at[pl.ds(base + at, STEP), :],
                up.at[pl.ds(at, STEP), :],
            ]

        def both_ways(make, carry):
            if near == 0:
                return lax.fori_loop(0, padded // STEP, make(None, 0), carry)
            carry = lax.fori_loop(0, near // STEP, make(outs[1], padded), carry)
            return lax.fori_loop(
                near // STEP, padded // STEP, make(outs[2], padded - near), carry
            )

        def copied(far, base):
            def some(i, highest):
                at = pl.multiple_of(i * STEP, 8)
                live = at + lax.broadcasted_iota(jnp.int32, (STEP, lanes), 0) < cols
                highest = list(highest)
                outputs = spots(at, far, base)
                for tile in range(2):
                    across = slice(tile * lanes, (tile + 1) * lanes)
                    both = half_swapped(
                        own_sum[pl.ds(at, STEP), across], other_sum[pl.ds(at, STEP), across], low
                    )
                    for k in range(2):
                        value = jnp.where(live, both[k], LOW)
                        outputs[2 * tile + k][...] = value
                        highest[2 * tile + k] = jnp.maximum(highest[2 * tile + k], value)
                return tuple(highest)

            return some

        highest = tuple(jnp.full((STEP, lanes), LOW, jnp.float32) for _ in range(4))
        highest = both_ways(copied, highest)
        top = [jnp.max(h, axis=0, keepdims=True) for h in highest]

        def summed(far, base):
            def some(i, totals):
                outputs = spots(pl.multiple_of(i * STEP, 8), far, base)
                return tuple(t + jnp.exp(g[...] - m) for t, g, m in zip(totals, outputs, top))

            return some

        totals = tuple(jnp.zeros((STEP, lanes), jnp.float32) for _ in range(4))
        totals = both_ways(summed, totals)
        stats[...] = before[...]
        for block in range(4):
            stats[goals[block], row : row + 1, :] = top[block]
            stats[goals[block], row + 2 : row + 3, :] = jnp.sum(totals[block], axis=0, keepdims=True)


def logits_of(pieces, dims, own_w, other_w, before, row, place, padded, near):
    cols = own_w.shape[0]
    nz, ny, nx = dims
    counts = [len(found) for found in pieces]
    arrays = [array for found in pieces for array, _ in found]
    rows, width = arrays[0].shape[-2:]
    lanes = 2 * rows

    weight = pl.BlockSpec((cols, ny * width), lambda k, s: (0, k))
    if near == 0:
        sizes = [(nx, padded, lanes)]
    else:
        sizes = [(padded, lanes), (padded + near, lanes), (2 * padded - near, lanes)]
    sizes.append(before.shape)

    def whole(shape):
        return pl.BlockSpec(shape, lambda k, s: (0,) * len(shape))

    def body(place, *refs):
        logits_kernel(nz, counts, cols, near, row, place, *refs)

    return pl.pallas_call(
        body,
        grid_spec=pltpu.PrefetchScalarGridSpec(
            num_scalar_prefetch=1,
            grid=(nz,),
            in_specs=[spec for found in pieces for _, spec in found]
            + [weight, weight, whole(before.shape)],
            out_specs=[whole(shape) for shape in sizes],
            scratch_shapes=[pltpu.VMEM((padded, nx * rows), jnp.float32)] * 2
            + [pltpu.VMEM((ny, nx * rows, width), jnp.bfloat16)],
        ),
        out_shape=[jax.ShapeDtypeStruct(shape, jnp.float32) for shape in sizes],
        cost_estimate=pl.CostEstimate(
            flops=4 * cols * nx * rows * width * ny * nz,
            bytes_accessed=(2 * cols + nx * rows) * width * ny * nz * 2,
            transcendentals=0,
        ),
        compiler_params=pltpu.CompilerParams(
            dimension_semantics=("arbitrary",), vmem_limit_bytes=52 << 20
        ),
        name="logits",
    )(place, *arrays, own_w, other_w, before)


def table_kernel(near, place, first, stay, up, far_up, far_down, down, stats, table):
    padded, lanes = stay.shape

    tops, totals = stats[:, 0:2, :], stats[:, 2:4, :]
    top = jnp.max(tops, axis=0)
    total = jnp.sum(jnp.exp(tops - top[None]) * totals, axis=0)
    swap = lanes // 2
    both = jnp.maximum(top, pltpu.roll(top, swap, 1))
    total = total * jnp.exp(top - both)
    total = total + pltpu.roll(total, swap, 1)
    one_low = lax.broadcasted_iota(jnp.int32, (1, lanes), 1) < swap
    highest = jnp.where(one_low, both[0:1, :], both[1:2, :])
    scale = 1.0 / jnp.where(one_low, total[0:1, :], total[1:2, :])
    low = lax.broadcasted_iota(jnp.int32, (STEP, lanes), 1) < swap

    def fill(away, second, begin, end, shift):
        source = lax.rem(place[2] + away, 4)

        def some(i, carry):
            at = pl.multiple_of(i * STEP, 8)
            a = first[source, pl.ds(at, STEP), :]
            b = second[pl.ds(at + shift, STEP), :]
            for side, value in enumerate(half_swapped(a, b, low)):
                value = (jnp.exp(value - highest) * scale).astype(jnp.bfloat16)
                goal = pl.multiple_of(source * (2 * padded) + side * padded + at, 8)
                table[pl.ds(goal, STEP), :] = value.astype(jnp.float32)
            return carry

        lax.fori_loop(begin // STEP, end // STEP, some, 0)

    fill(0, stay, 0, padded, 0)
    fill(1, up, 0, padded, 0)
    fill(2, far_up, 0, near, 0)
    fill(2, far_down, near, padded, -near)
    fill(3, down, 0, padded, 0)
    table[8 * padded : 8 * padded + 8, :] = jnp.zeros((8, lanes), jnp.float32)


def table_of(place, first, second, stats, near):
    padded, lanes = second[0].shape
    vmem = pl.BlockSpec(memory_space=pltpu.VMEM)

    def body(*refs):
        table_kernel(near, *refs)

    return pl.pallas_call(
        body,
        in_specs=[pl.BlockSpec(memory_space=pltpu.SMEM)] + [vmem] * 7,
        out_specs=vmem,
        out_shape=jax.ShapeDtypeStruct((8 * padded + 8, lanes), jnp.float32),
        name="table",
    )(place, first, *second, stats)


def gather_kernel(index, table, out, wide):
    def some(i, carry):
        base = pl.multiple_of(i * 32, 32)
        for k in range(32):
            wide[k : k + 1, :] = table[pl.ds(index[base + k], 1), :]
        out[pl.ds(base, 32), :] = wide[...].astype(out.dtype)
        return carry

    lax.fori_loop(0, out.shape[0] // 32, some, 0)


def rows_of(table, index):
    lanes = table.shape[1]
    return pl.pallas_call(
        gather_kernel,
        in_specs=[
            pl.BlockSpec(memory_space=pltpu.SMEM),
            pl.BlockSpec(memory_space=pltpu.VMEM),
        ],
        out_specs=pl.BlockSpec(memory_space=pltpu.VMEM),
        out_shape=jax.ShapeDtypeStruct((index.shape[0], lanes), jnp.bfloat16),
        scratch_shapes=[pltpu.VMEM((32, lanes), jnp.float32)],
        cost_estimate=pl.CostEstimate(
            flops=index.shape[0] * 800000, bytes_accessed=index.shape[0] * lanes * 6, transcendentals=0
        ),
        name="rows",
    )(index, table)


def scatter_kernel(began, target, values, *refs):
    before, out, wide, sums = refs[: int(began)], refs[int(began)], refs[-ACCS - 1], refs[-ACCS:]
    rows, lanes = out.shape

    def widened(i, carry):
        at = pl.multiple_of(i * 128, 32)
        wide[pl.ds(at, 128), :] = values[pl.ds(at, 128), :].astype(jnp.float32)
        return carry

    lax.fori_loop(0, values.shape[0] // 128, widened, 0)

    def cleared(i, carry):
        for total in sums:
            total[pl.ds(pl.multiple_of(i * 96, 8), 96), :] = jnp.zeros((96, lanes), jnp.float32)
        return carry

    lax.fori_loop(0, sums[0].shape[0] // 96, cleared, 0)

    def some(i, carry):
        base = i * (2 * ACCS)
        for turn in range(2):
            at = [target[base + turn * ACCS + k] for k in range(ACCS)]
            new = [
                total[pl.ds(at[k], 1), :] + wide[pl.ds(base + turn * ACCS + k, 1), :]
                for k, total in enumerate(sums)
            ]
            for k, total in enumerate(sums):
                total[pl.ds(at[k], 1), :] = new[k]
        return carry

    lax.fori_loop(0, values.shape[0] // (2 * ACCS), some, 0)

    def gathered(start, size):
        at = pl.ds(start, size)
        parts = [total[at, :] for total in sums]
        while len(parts) > 1:
            parts = [a + b for a, b in zip(parts[::2], parts[1::2])]
        out[at, :] = parts[0] + before[0][at, :] if began else parts[0]

    def some_gathered(i, carry):
        gathered(pl.multiple_of(i * 80, 8), 80)
        return carry

    lax.fori_loop(0, rows // 80, some_gathered, 0)
    if rows % 80:
        gathered(rows // 80 * 80, rows % 80)


def added_rows(values, target, rows, before):
    lanes = values.shape[1]
    began = before is not None
    vmem = pl.BlockSpec(memory_space=pltpu.VMEM)

    def body(*refs):
        scatter_kernel(began, *refs)

    return pl.pallas_call(
        body,
        in_specs=[pl.BlockSpec(memory_space=pltpu.SMEM), vmem] + [vmem] * int(began),
        out_specs=vmem,
        out_shape=jax.ShapeDtypeStruct((rows, lanes), jnp.float32),
        scratch_shapes=[pltpu.VMEM(values.shape, jnp.float32)]
        + [pltpu.VMEM((-(-(rows + 8) // 96) * 96, lanes), jnp.float32)] * ACCS,
        cost_estimate=pl.CostEstimate(
            flops=values.shape[0] * 1000000, bytes_accessed=values.shape[0] * lanes * 6, transcendentals=0
        ),
        name="folded",
    )(target, values, *([before] if began else []))


def from_all(value, axes):
    copies = jnp.broadcast_to(value, (lax.axis_size(axes), *value.shape))
    return lax.all_to_all(copies, axes, split_axis=0, concat_axis=0, tiled=True)


def shards(hidden_rows, teacher_weight, student_logits, slot_source, slot_target):
    x, core = lax.axis_index("tok_0"), lax.axis_index("tok_1")
    z, y = lax.axis_index("voc_0"), lax.axis_index("voc_1")
    cols = teacher_weight.shape[1]
    padded = -(-cols // 8) * 8
    own_w = teacher_weight.T
    other_w = lax.ppermute(own_w, "tok_1", [(0, 1), (1, 0)])

    half = hidden_rows.shape[0] // 2
    nz, ny, nx = (lax.axis_size(name) for name in ("voc_0", "voc_1", "tok_0"))
    dims = (nz, ny, nx)
    second = from_all(hidden_rows[half:], "voc_0")
    first = stacked(ring(hidden_rows[:half], "tok_0"))
    second = stacked(ring(second, "tok_0"))
    first = from_all(first, "voc_1")
    first = stacked(ring(first, "voc_0"))
    second = ring(second, "voc_1")
    rows, width = half, hidden_rows.shape[1]

    def first_piece(j):
        return pl.BlockSpec(
            (1, 1, nx, rows, width), lambda k, s: (lax.rem(k + nz - s[0], nz), j, 0, 0, 0)
        )

    first = [[(first, first_piece(j))] for j in range(ny)]
    second = [
        [
            (part, pl.BlockSpec((part.shape[0], 1, rows, width), lambda k, s: (0, k, 0, 0)))
            for part in found
        ]
        for found in second
    ]

    student = student_logits.T.astype(jnp.float32)
    student_max = jnp.max(student, axis=0)
    student_total = jnp.sum(jnp.exp(student - student_max[None]), axis=0)
    lanes = student.shape[1]
    none = jnp.zeros((lanes,), jnp.float32)
    stats = jnp.stack([none, none, none, none, student_max, student_total, none, none])
    stats = jnp.broadcast_to(stats, (nx, *stats.shape))
    place = jnp.stack([z, y, x]).astype(jnp.int32)
    near = (padded // STEP + 1) // 2 * STEP
    first, stats = logits_of(
        first, dims, own_w, other_w, stats, 0, place, padded, 0
    )
    first = lax.all_to_all(first, "tok_0", 0, 0, tiled=True)
    stay, up, down, stats = logits_of(second, dims, own_w, other_w, stats, 1, place, padded, near)
    owners, slots = slot_source.shape[1:]
    stats = jnp.broadcast_to(stats[:, None], (nx, owners, *stats.shape[1:]))
    stats = stats.reshape(-1, *stats.shape[2:])
    up = from_neighbour(up, "tok_0", 1)
    down = from_neighbour(down, "tok_0", -1)
    stats = lax.all_to_all(stats, ("tok_0", *VOC), 0, 0, tiled=True)
    far_up = from_neighbour(up[padded:], "tok_0", 1)
    far_down = from_neighbour(down[padded:], "tok_0", -1)
    table = table_of(place, first, (stay, up, far_up, far_down, down), stats, near)
    own = lax.dynamic_slice_in_dim(stats, x * owners, owners, 0)
    highest = jnp.max(own[:, 4], axis=0)
    student_lse = highest + jnp.log(
        jnp.sum(own[:, 5] * jnp.exp(own[:, 4] - highest[None]), axis=0)
    )

    source = slot_source[0]
    shard = jnp.maximum(source, 0) // cols
    local = jnp.maximum(source, 0) - shard * cols
    block = shard // 2
    side = (shard % 2) ^ core
    index = jnp.where(source >= 0, block * (2 * padded) + side * padded + local, 8 * padded)
    width = student_logits.shape[1]
    target = jnp.where(slot_target[0] >= 0, slot_target[0], width)
    some = slots // CHUNKS

    def slots_of(value, i):
        return value[:, i * some : (i + 1) * some].reshape(-1).astype(jnp.int32)

    folded = None
    for i in range(CHUNKS):
        picked = rows_of(table, slots_of(index, i)).reshape(owners, some, lanes)
        arrived = lax.all_to_all(picked, VOC, split_axis=0, concat_axis=0, tiled=True)
        folded = added_rows(arrived.reshape(-1, lanes), slots_of(target, i), width, folded)

    sums = from_all(jnp.stack([jnp.sum(folded * student, axis=0), jnp.sum(folded, axis=0)]), VOC)
    student_grad = (jnp.exp(student - student_lse[None]) - folded).astype(jnp.bfloat16)
    sums, student_grad = lax.optimization_barrier((sums, student_grad))
    cross, mass = jnp.sum(sums[:, 0], axis=0), jnp.sum(sums[:, 1], axis=0)
    loss = student_lse * mass - cross
    return (loss, student_grad.T)


def solution(mesh):
    finer = Mesh(mesh.devices.reshape(4, 2, 8, 4), ("tok_0", "tok_1", "voc_0", "voc_1"))
    placed = (P(TOK, VOC), P(None, TOK_VOC), P(TOK, VOC), P(VOC, None, None), P(VOC, None, None))

    return jax.shard_map(
        shards, mesh=finer, in_specs=placed, out_specs=(P(TOK), P(TOK, VOC)), check_vma=False
    )
```
